32 devices in a mesh: rep: 4 (over y, x), fsdp: 8 (over z, core).
Axes of the slice: x: 2, y: 2, z: 4, core: 2. Of those that a mesh axis runs over, the one named last changes fastest.
Arguments:
- inputs: bfloat16 [32, 1024, 768], P(('rep', 'fsdp')), may hold values from -6 to 6
- w_query: bfloat16 [768, 768], P('fsdp'), may hold values from -0.21875 to 0.21875
- w_key: bfloat16 [768, 768], P('fsdp'), may hold values from -0.21875 to 0.21875
- w_value: bfloat16 [768, 768], P('fsdp'), may hold values from -0.21875 to 0.21875
- w_out: bfloat16 [768, 768], P('fsdp'), may hold values from -0.875 to 0.875
- w_gate: bfloat16 [768, 2048], P('fsdp'), may hold values from -0.21875 to 0.21875
- w_up: bfloat16 [768, 2048], P('fsdp'), may hold values from -0.21875 to 0.21875
- w_down: bfloat16 [2048, 768], P('fsdp'), may hold values from -0.125 to 0.125
- norm_attn: bfloat16 [768], P('fsdp'), may hold values from 0.25 to 1.75
- norm_ffn: bfloat16 [768], P('fsdp'), may hold values from 0.25 to 1.75
- lengths: int32 [32], P(('rep', 'fsdp')), may hold values from 64 to 1024, as said below
- cotangent: bfloat16 [32, 1024, 768], P(('rep', 'fsdp')), may hold values from -6 to 6
Outputs:
- output: bfloat16 [32, 1024, 768], P(('rep', 'fsdp'))
- grad_input: bfloat16 [32, 1024, 768], P(('rep', 'fsdp'))
- grad_query: float32 [768, 768], P('fsdp')
- grad_key: float32 [768, 768], P('fsdp')
- grad_value: float32 [768, 768], P('fsdp')
- grad_out: float32 [768, 768], P('fsdp')
- grad_gate: float32 [768, 2048], P('fsdp')
- grad_up: float32 [768, 2048], P('fsdp')
- grad_down: float32 [2048, 768], P('fsdp')
- grad_norm_attn: float32 [768], P('fsdp')
- grad_norm_ffn: float32 [768], P('fsdp')
The draws below stay inside these ranges and needn't reach their ends.
Inputs may be any that keep to these rules, and one draw needn't show every extreme that they name: Tokens at positions lengths[s] and beyond are padding. Some sequence has exactly 1024 valid tokens.
All inputs are finite; a program needn't handle non-finite values.
Results may differ from the reference program's by a relative error of at most 0.018.
Values may be sent and summed in bfloat16 or wider, within the bound.
No kernel may reach another device: no remote copies, remote signals or barrier semaphores. Data moves between devices by JAX's collectives and lax.ppermute only.
A program may use at most 192 MiB of HBM per device.

```python
import math
import jax
import jax.numpy as jnp
from jax import lax

D = 768
HEADS = 12
HEAD_DIM = 64
FF = 2048
SEQ_LEN = 1024
SEQS = 32


def draw_lengths(key, part):
    first_key, second_key, third_key = jax.random.split(key, 3)
    levels = jax.random.randint(first_key, (SEQS,), 0, 5)
    base_len = jnp.left_shift(jnp.full((SEQS,), SEQ_LEN // 16, jnp.int32), levels)
    extra = jax.random.randint(second_key, (SEQS,), 0, 1073741824) % base_len
    drawn = jnp.minimum(base_len + extra, SEQ_LEN)
    chosen = jax.random.randint(third_key, (), 0, SEQS)
    return drawn.at[chosen].set(SEQ_LEN).astype(jnp.int32)


def level_of(stream_key, shape, cuts, low, top_value):
    loudness = 1.0
    for axis_at, shards_of in cuts:
        steps = jax.random.uniform(jax.random.fold_in(jax.random.fold_in(stream_key, 6), axis_at), (shards_of,), jnp.float32, low / len(cuts), top_value / len(cuts))
        loudness = loudness * jnp.repeat(jnp.exp(steps), shape[axis_at] // shards_of).reshape((-1,) + (1,) * (len(shape) - 1 - axis_at))
    return loudness


def bell_draw(key, shape, width, limit, shards=(), kind=jnp.bfloat16):
    array = jax.random.normal(key, shape, jnp.float32) * width
    if len(shards) > 0:
        array = level_of(key, shape, shards, -0.22, 0.18) * array
    return jnp.clip(array, min=-limit, max=limit).astype(kind)


def setup_inputs(seed: int = 0) -> dict:
    splits = jax.random.split(jax.random.key(seed), 13)
    inputs = bell_draw(splits[0], (SEQS, SEQ_LEN, D), 1.0, 6.0, ((0, 32),))
    w_query = bell_draw(splits[1], (D, D), D ** -0.5, 0.21875, ((0, 8),))
    w_key = bell_draw(splits[2], (D, D), D ** -0.5, 0.21875, ((0, 8),))
    w_value = bell_draw(splits[3], (D, D), D ** -0.5, 0.21875, ((0, 8),))
    w_out = bell_draw(splits[4], (D, D), (D // 16) ** -0.5, 0.875, ((0, 8),))
    w_gate = bell_draw(splits[5], (D, FF), D ** -0.5, 0.21875, ((0, 8),))
    w_up = bell_draw(splits[6], (D, FF), D ** -0.5, 0.21875, ((0, 8),))
    w_down = bell_draw(splits[7], (FF, D), FF ** -0.5, 0.125, ((0, 8),))
    norm_attn = jnp.clip(1.0 + 0.15 * jax.random.normal(splits[8], (D,), jnp.float32), 0.25, 1.75).astype(jnp.bfloat16)
    norm_ffn = jnp.clip(1.0 + 0.15 * jax.random.normal(splits[9], (D,), jnp.float32), 0.25, 1.75).astype(jnp.bfloat16)
    lengths = draw_lengths(jax.random.fold_in(splits[12], 71), 0)
    cotangent = bell_draw(splits[11], (SEQS, SEQ_LEN, D), 1.0, 6.0, ((0, 32),))
    return dict(inputs=inputs, w_query=w_query, w_key=w_key, w_value=w_value, w_out=w_out, w_gate=w_gate, w_up=w_up, w_down=w_down, norm_attn=norm_attn, norm_ffn=norm_ffn, lengths=lengths, cotangent=cotangent)


@jax.custom_vjp
def low(v):
    return lax.optimization_barrier(v.astype(jnp.bfloat16)).astype(jnp.float32)

@jax.custom_vjp
def low_back(v):
    return v

def low_keep(v):
    return (low(v), None)

def low_pass(kept, grad):
    return (grad,)

def back_keep(v):
    return (v, None)

def back_low(kept, grad):
    return (low(grad),)
low.defvjp(low_keep, low_pass)
low_back.defvjp(back_keep, back_low)
EPSILON = 1e-05
HIGHEST = lax.Precision.HIGHEST

def rotary_tables(seq_length, head_width):
    half_width = head_width // 2
    position = jnp.arange(seq_length, dtype=jnp.float32)
    inverse = 10000.0 ** (-(jnp.arange(half_width, dtype=jnp.float32) * 2.0 / head_width))
    angles = position[:, None] * inverse[None, :]
    return (jnp.cos(angles), jnp.sin(angles))

def rotate(values, cosine, sine_table):
    half_width = values.shape[-1] // 2
    former = values[..., :half_width]
    latter = values[..., half_width:]
    return jnp.concatenate([former * cosine - latter * sine_table, latter * cosine + former * sine_table], axis=-1)

def rms_norm(values, gain):
    return values * lax.rsqrt(lax.optimization_barrier(jnp.mean(values * values, axis=-1, keepdims=True)) + EPSILON) * gain

def project(left, right):
    return jnp.einsum('gld,de->gle', left, right, precision=HIGHEST)

def block_forward(inputs, w_query, w_key, w_value, w_out, w_gate, w_up, w_down, norm_attn, norm_ffn, allowed):
    seq_count = inputs.shape[0]
    cosine, sine_table = rotary_tables(SEQ_LEN, HEAD_DIM)
    cosine = cosine[:, None, :]
    sine_table = sine_table[:, None, :]
    shape_heads = (seq_count, SEQ_LEN, HEADS, HEAD_DIM)
    normed = low(rms_norm(inputs, norm_attn))
    queries = low(rotate(low_back(project(normed, w_query)).reshape(shape_heads), cosine, sine_table))
    keys_rot = low(rotate(low_back(project(normed, w_key)).reshape(shape_heads), cosine, sine_table))
    values_all = low(low_back(project(normed, w_value))).reshape(shape_heads)
    scores = low_back(jnp.einsum('gqhe,gkhe->ghqk', queries, keys_rot, precision=HIGHEST) * HEAD_DIM ** (-0.5))
    scores = jnp.where(allowed[:, None, :, :], scores, -1e+30)
    attention = low(jax.nn.softmax(scores, axis=-1))
    mixed = jnp.einsum('ghqk,gkhe->gqhe', attention, values_all, precision=HIGHEST)
    mixed = low(low_back(mixed)).reshape(seq_count, SEQ_LEN, D)
    residual = inputs + low_back(project(mixed, w_out))
    normed_ffn = low(rms_norm(residual, norm_ffn))
    gate_proj = low_back(project(normed_ffn, w_gate))
    up_proj = low_back(project(normed_ffn, w_up))
    hidden = low(jax.nn.silu(gate_proj) * up_proj)
    return residual + low_back(project(hidden, w_down))

def reference(inputs, w_query, w_key, w_value, w_out, w_gate, w_up, w_down, norm_attn, norm_ffn, lengths, cotangent):
    weights = tuple((weight_item.astype(jnp.float32) for weight_item in (w_query, w_key, w_value, w_out, w_gate, w_up, w_down, norm_attn, norm_ffn)))
    seq_total = inputs.shape[0]
    per_step = math.gcd(seq_total, max(1, 2048 // SEQ_LEN))
    step_count = seq_total // per_step
    position = jnp.arange(SEQ_LEN, dtype=jnp.int32)
    causal = position[None, :] <= position[:, None]
    valid_rows = (position[None, :] < lengths[:, None]).astype(jnp.float32)
    seeds = cotangent.astype(jnp.float32) * valid_rows[:, :, None]
    grouped = (inputs.astype(jnp.float32).reshape(step_count, per_step, SEQ_LEN, D), lengths.reshape(step_count, per_step), seeds.reshape(step_count, per_step, SEQ_LEN, D))

    def one_step(running, operand):
        block_in, block_len, block_seed = operand
        allowed = causal[None, :, :] & (position[None, None, :] < block_len[:, None, None])

        def forward(block_x, *params):
            return block_forward(block_x, *params, allowed)
        result, pullback = jax.vjp(forward, block_in, *weights)
        grad_terms = pullback(block_seed)
        return (tuple((sofar + increment for sofar, increment in zip(running, grad_terms[1:]))), (result, grad_terms[0]))
    start = tuple((jnp.zeros(weight_item.shape, jnp.float32) for weight_item in weights))
    reduced, (results, grad_in) = lax.scan(one_step, start, grouped)
    return (results.reshape(inputs.shape).astype(jnp.bfloat16), grad_in.reshape(inputs.shape).astype(jnp.bfloat16), reduced[0], reduced[1], reduced[2], reduced[3], reduced[4], reduced[5], reduced[6], reduced[7], reduced[8])
```

```python
import functools

import jax
import jax.numpy as jnp
import numpy as np
from jax import lax
from jax.experimental import pallas as pl
from jax.experimental.pallas import tpu as pltpu
from jax.sharding import PartitionSpec as P

HEADS = 12
EPSILON = 1e-05
F32 = jnp.float32
BF16 = jnp.bfloat16
NEG = -1e30
VMEM_LIMIT = 56 * 1024 * 1024

NN = (((1,), (0,)), ((), ()))
NT = (((1,), (1,)), ((), ()))


def mm(a, b, dims=NN):
    return lax.dot_general(a, b, dims, preferred_element_type=F32)


def params():
    return pltpu.CompilerParams(
        dimension_semantics=("arbitrary",), vmem_limit_bytes=VMEM_LIMIT
    )


def cost(flops, nbytes, exps=0):
    return pl.CostEstimate(flops=int(flops), bytes_accessed=int(nbytes), transcendentals=int(exps))


def rotary_lanes(seq_length, head_width):
    half = head_width // 2
    inverse = 10000.0 ** (-(np.arange(half, dtype=np.float64) * 2.0 / head_width))
    angles = np.arange(seq_length, dtype=np.float64)[:, None] * inverse[None, :]
    cos = np.cos(angles)
    sin = np.sin(angles)
    return (
        np.concatenate([cos] * 4, axis=1).astype(np.float32),
        np.concatenate([-sin, sin, -sin, sin], axis=1).astype(np.float32),
    )


def turn(y, cos, sin):
    lane = lax.broadcasted_iota(jnp.int32, y.shape, 1)
    first = (lane % 64) < 32
    other = jnp.where(first, pltpu.roll(y, 96, 1), pltpu.roll(y, 32, 1))
    return y * cos + other * sin


def rms_row(x):
    return lax.rsqrt(jnp.mean(x * x, axis=-1, keepdims=True) + EPSILON)


def qkv_body(x_ref, g_ref, w_ref, cos_ref, sin_ref, h_ref, q_ref, k_ref, v_ref):
    x = x_ref[...].astype(F32)
    h = (x * rms_row(x) * g_ref[...].astype(F32)).astype(BF16)
    h_ref[...] = h
    cos = cos_ref[...]
    sin = sin_ref[...]
    for i, out in ((0, q_ref), (1, k_ref)):
        y = mm(h, w_ref[i])
        for c in range(y.shape[1] // 128):
            s = slice(128 * c, 128 * c + 128)
            out[:, s] = turn(y[:, s], cos, sin).astype(BF16)
    v_ref[...] = mm(h, w_ref[2]).astype(BF16)


def qkv_forward(x, gain, wqkv, cos, sin):
    rows, d = x.shape
    rb = 256
    row = pl.BlockSpec((rb, d), lambda i: (i, 0))
    tab = pl.BlockSpec((rb, 128), lambda i: (i, 0))
    out = jax.ShapeDtypeStruct((rows, d), BF16)
    return pl.pallas_call(
        qkv_body,
        grid=(rows // rb,),
        in_specs=[
            row,
            pl.BlockSpec((1, d), lambda i: (0, 0)),
            pl.BlockSpec((3, d, d), lambda i: (0, 0, 0)),
            tab,
            tab,
        ],
        out_specs=[row] * 4,
        out_shape=[out] * 4,
        compiler_params=params(),
        cost_estimate=cost(6 * rows * d * d, 10 * rows * d + 6 * d * d),
        name="qkv",
    )(x, gain, wqkv, cos, sin)


def head_parts(length, q_ref, k_ref, h, q_aug, q_raw, k_aug):
    seq = q_ref.shape[0]
    lane = lax.broadcasted_iota(jnp.int32, (seq, 128), 1)
    row = lax.broadcasted_iota(jnp.int32, (seq, 128), 0)
    mine = (lane // 64) == h
    spare = lane == 64 * (1 - h)
    q = jnp.where(mine, q_ref[...].astype(F32) * 0.125, 0.0)
    if q_raw is not None:
        q_raw[...] = q.astype(BF16)
    q_aug[...] = jnp.where(spare, 1.0, q).astype(BF16)
    mask = jnp.where(spare & (row >= length), NEG, 0.0)
    k_aug[...] = jnp.where(mine, k_ref[...].astype(F32), mask).astype(BF16)


def attn_fwd_body(len_ref, q_ref, k_ref, v_ref, o_ref, lse_ref, q_aug, k_aug, vt, ot):
    length = len_ref[0]
    seq = q_ref.shape[0]
    qb = 256
    vt[...] = v_ref[...].T
    key = lax.broadcasted_iota(jnp.int32, (qb, qb), 0)
    qry = lax.broadcasted_iota(jnp.int32, (qb, qb), 1)
    for h in range(2):
        head_parts(length, q_ref, k_ref, h, q_aug, None, k_aug)
        hs = slice(64 * h, 64 * h + 64)
        for i in range(seq // qb):
            lo, hi = qb * i, qb * i + qb
            q = q_aug[lo:hi, :]
            diag = mm(k_aug[lo:hi, :], q, NT)
            diag = jnp.where(key <= qry, diag, NEG)
            top = jnp.max(diag, axis=0, keepdims=True)
            if lo:
                past = mm(k_aug[:lo, :], q, NT)
                top = jnp.maximum(top, jnp.max(past, axis=0, keepdims=True))
            pd = jnp.exp(diag - top)
            total = jnp.sum(pd, axis=0, keepdims=True)
            acc = mm(vt[hs, lo:hi], pd.astype(BF16))
            if lo:
                pp = jnp.exp(past - top)
                total = total + jnp.sum(pp, axis=0, keepdims=True)
                acc = acc + mm(vt[hs, :lo], pp.astype(BF16))
            ot[hs, lo:hi] = acc / total
            lse_ref[0, h : h + 1, lo:hi] = top + jnp.log(total)
    o_ref[...] = ot[...].T.astype(BF16)


def attention_forward(length, q, k, v):
    seq, d = q.shape
    pairs = d // 128
    col = pl.BlockSpec((seq, 128), lambda p: (0, p))
    return pl.pallas_call(
        attn_fwd_body,
        grid=(pairs,),
        in_specs=[pl.BlockSpec(memory_space=pltpu.SMEM), col, col, col],
        out_specs=[col, pl.BlockSpec((1, 2, seq), lambda p: (p, 0, 0))],
        out_shape=[
            jax.ShapeDtypeStruct((seq, d), BF16),
            jax.ShapeDtypeStruct((pairs, 2, seq), F32),
        ],
        scratch_shapes=[
            pltpu.VMEM((seq, 128), BF16),
            pltpu.VMEM((seq, 128), BF16),
            pltpu.VMEM((128, seq), BF16),
            pltpu.VMEM((128, seq), F32),
        ],
        compiler_params=params(),
        cost_estimate=cost(16 * seq * seq * d, 8 * seq * d, seq * seq * pairs),
        name="attn_fwd",
    )(length, q, k, v)


def attn_bwd_body(
    len_ref, q_ref, k_ref, v_ref, o_ref, go_ref, lse_ref, cos_ref, sin_ref, g_ref,
    qa0, qa1, qz0, qz1, ka0, ka1, gz0, gz1, kt, et, dqt,
):
    length = len_ref[0]
    seq = q_ref.shape[0]
    kb = 256
    qa, qz, ka, gz = (qa0, qa1), (qz0, qz1), (ka0, ka1), (gz0, gz1)
    go = go_ref[...].astype(F32)
    et[...] = (go * o_ref[...].astype(F32)).T
    kt[...] = k_ref[...].T
    lane = lax.broadcasted_iota(jnp.int32, (seq, 128), 1)
    deltas = []
    for h in range(2):
        head_parts(length, q_ref, k_ref, h, qa[h], qz[h], ka[h])
        gz[h][...] = jnp.where((lane // 64) == h, go, 0.0).astype(BF16)
        deltas.append(jnp.sum(et[64 * h : 64 * h + 64, :], axis=0, keepdims=True))
    key = lax.broadcasted_iota(jnp.int32, (kb, kb), 0)
    qry = lax.broadcasted_iota(jnp.int32, (kb, kb), 1)
    causal = key <= qry
    for j in range(seq // kb):
        lo, hi = kb * j, kb * j + kb
        dv = None
        dk = None
        v = v_ref[lo:hi, :]
        for h in range(2):
            hs = slice(64 * h, 64 * h + 64)
            k = ka[h][lo:hi, :]
            parts = [(lo, hi)] + ([(hi, seq)] if hi < seq else [])
            for n, (a, b) in enumerate(parts):
                s = mm(k, qa[h][a:b, :], NT)
                p = jnp.exp(s - lse_ref[0, h : h + 1, a:b])
                if n == 0:
                    p = jnp.where(causal, p, 0.0)
                dp = mm(v, gz[h][a:b, :], NT)
                ds = (p * (dp - deltas[h][:, a:b])).astype(BF16)
                pb = p.astype(BF16)
                tv = mm(pb, gz[h][a:b, :])
                tk = mm(ds, qz[h][a:b, :])
                tq = mm(kt[hs, lo:hi], ds)
                dv = tv if dv is None else dv + tv
                dk = tk if dk is None else dk + tk
                if j == 0:
                    dqt[hs, a:b] = tq
                else:
                    dqt[hs, a:b] += tq
        g_ref[2, lo:hi, :] = dv.astype(BF16)
        g_ref[1, lo:hi, :] = turn(dk, cos_ref[lo:hi, :], -sin_ref[lo:hi, :]).astype(BF16)
    dq = dqt[...].T * 0.125
    g_ref[0] = turn(dq, cos_ref[...], -sin_ref[...]).astype(BF16)


def attention_backward(length, q, k, v, o, go, lse, cos, sin, first, count):
    seq, d = q.shape
    col = pl.BlockSpec((seq, 128), lambda p: (0, p + first))
    tab = pl.BlockSpec((seq, 128), lambda p: (0, 0))
    wide = pltpu.VMEM((seq, 128), BF16)
    return pl.pallas_call(
        attn_bwd_body,
        grid=(count,),
        in_specs=[pl.BlockSpec(memory_space=pltpu.SMEM)]
        + [col] * 5
        + [pl.BlockSpec((1, 2, seq), lambda p: (p + first, 0, 0)), tab, tab],
        out_specs=pl.BlockSpec((3, seq, 128), lambda p: (0, 0, p)),
        out_shape=jax.ShapeDtypeStruct((3, seq, count * 128), BF16),
        scratch_shapes=[wide] * 8
        + [
            pltpu.VMEM((128, seq), BF16),
            pltpu.VMEM((128, seq), F32),
            pltpu.VMEM((128, seq), F32),
        ],
        compiler_params=params(),
        cost_estimate=cost(40 * seq * seq * 128 * count, 16 * seq * 128 * count, seq * seq * count),
        name="attn_bwd",
    )(length, q, k, v, o, go, lse, cos, sin)


def out_body(len_ref, x_ref, o_ref, w_ref, g_ref, ct_ref, x1_ref, h2_ref, gy_ref):
    x1 = x_ref[...].astype(F32) + mm(o_ref[...], w_ref[...])
    x1_ref[...] = x1
    h2_ref[...] = (x1 * rms_row(x1) * g_ref[...].astype(F32)).astype(BF16)
    rb = x1.shape[0]
    row = lax.broadcasted_iota(jnp.int32, x1.shape, 0) + pl.program_id(0) * rb
    gy_ref[...] = jnp.where(row < len_ref[0], ct_ref[...].astype(F32), 0.0).astype(BF16)


def out_forward(length, x, o, w, gain, ct):
    rows, d = x.shape
    rb = 256
    row = pl.BlockSpec((rb, d), lambda i: (i, 0))
    return pl.pallas_call(
        out_body,
        grid=(rows // rb,),
        in_specs=[
            pl.BlockSpec(memory_space=pltpu.SMEM),
            row,
            row,
            pl.BlockSpec((d, d), lambda i: (0, 0)),
            pl.BlockSpec((1, d), lambda i: (0, 0)),
            row,
        ],
        out_specs=[row] * 3,
        out_shape=[
            jax.ShapeDtypeStruct((rows, d), F32),
            jax.ShapeDtypeStruct((rows, d), BF16),
            jax.ShapeDtypeStruct((rows, d), BF16),
        ],
        compiler_params=params(),
        cost_estimate=cost(2 * rows * d * d, 14 * rows * d),
        name="out_fwd",
    )(length, x, o, w, gain, ct)


def ffn_body(h_ref, gy_ref, x1_ref, wg_ref, wu_ref, wd_ref,
             out_ref, gh_ref, gwg_ref, gwu_ref, gwd_ref, ht, acc):
    step = pl.program_id(0)

    @pl.when(step == 0)
    def _():
        ht[...] = h_ref[...].T
        acc[...] = x1_ref[...]
        gh_ref[...] = jnp.zeros_like(gh_ref)

    h = h_ref[...]
    gy = gy_ref[...]
    wg = wg_ref[...]
    wu = wu_ref[...]
    wd = wd_ref[...]
    gate = mm(h, wg)
    up = mm(h, wu)
    g_hidden = mm(gy, wd, NT)
    sig = jax.nn.sigmoid(gate)
    silu = gate * sig
    hidden = (silu * up).astype(BF16)
    g_gate = (g_hidden * up * sig * (1.0 + gate * (1.0 - sig))).astype(BF16)
    g_up = (g_hidden * silu).astype(BF16)
    acc[...] += mm(hidden, wd)
    gwd_ref[...] = mm(hidden.T, gy).astype(BF16)
    gwg_ref[...] = mm(ht[...], g_gate).astype(BF16)
    gwu_ref[...] = mm(ht[...], g_up).astype(BF16)
    gh_ref[...] += mm(g_gate, wg, NT) + mm(g_up, wu, NT)

    @pl.when(step == pl.num_programs(0) - 1)
    def _():
        out_ref[...] = acc[...].astype(BF16)


def ffn(h2, gy, x1, wg, wu, wd):
    rows, d = h2.shape
    width = wg.shape[1]
    fb = 256
    full = pl.BlockSpec((rows, d), lambda i: (0, 0))
    colw = pl.BlockSpec((d, fb), lambda i: (0, i))
    roww = pl.BlockSpec((fb, d), lambda i: (i, 0))
    return pl.pallas_call(
        ffn_body,
        grid=(width // fb,),
        in_specs=[full, full, full, colw, colw, roww],
        out_specs=[full, full, colw, colw, roww],
        out_shape=[
            jax.ShapeDtypeStruct((rows, d), BF16),
            jax.ShapeDtypeStruct((rows, d), F32),
            jax.ShapeDtypeStruct((d, width), BF16),
            jax.ShapeDtypeStruct((d, width), BF16),
            jax.ShapeDtypeStruct((width, d), BF16),
        ],
        scratch_shapes=[pltpu.VMEM((d, rows), BF16), pltpu.VMEM((rows, d), F32)],
        compiler_params=params(),
        cost_estimate=cost(18 * rows * d * width, 14 * rows * d + 12 * d * width, rows * width),
        name="ffn",
    )(h2, gy, x1, wg, wu, wd)


def out_bwd_body(gh_ref, x1_ref, gy_ref, o_ref, w_ref, g_ref,
                 gx_ref, go_ref, gw_ref, gn_ref, acc):
    step = pl.program_id(0)

    @pl.when(step == 0)
    def _():
        acc[...] = jnp.zeros_like(acc)
        gn_ref[...] = jnp.zeros_like(gn_ref)

    x1 = x1_ref[...]
    r = rms_row(x1)
    n = x1 * r
    gh = gh_ref[...]
    gn_ref[...] += jnp.sum(gh * n, axis=0, keepdims=True)
    s = gh * g_ref[...].astype(F32)
    gx = gy_ref[...].astype(F32) + r * (s - n * jnp.mean(s * n, axis=-1, keepdims=True))
    gx_ref[...] = gx
    ga = gx.astype(BF16)
    go_ref[...] = mm(ga, w_ref[...], NT).astype(BF16)
    acc[...] += mm(o_ref[...].T, ga)

    @pl.when(step == pl.num_programs(0) - 1)
    def _():
        gw_ref[...] = acc[...].astype(BF16)


def out_backward(gh, x1, gy, o, w, gain):
    rows, d = x1.shape
    rb = 256
    row = pl.BlockSpec((rb, d), lambda i: (i, 0))
    mat = pl.BlockSpec((d, d), lambda i: (0, 0))
    vec = pl.BlockSpec((1, d), lambda i: (0, 0))
    return pl.pallas_call(
        out_bwd_body,
        grid=(rows // rb,),
        in_specs=[row, row, row, row, mat, vec],
        out_specs=[row, row, mat, vec],
        out_shape=[
            jax.ShapeDtypeStruct((rows, d), F32),
            jax.ShapeDtypeStruct((rows, d), BF16),
            jax.ShapeDtypeStruct((d, d), BF16),
            jax.ShapeDtypeStruct((1, d), F32),
        ],
        scratch_shapes=[pltpu.VMEM((d, d), F32)],
        compiler_params=params(),
        cost_estimate=cost(4 * rows * d * d, 18 * rows * d),
        name="out_bwd",
    )(gh, x1, gy, o, w, gain)


def wgrad_body(h_ref, g_ref, gw_ref, ht):
    @pl.when(pl.program_id(0) == 0)
    def _():
        ht[...] = h_ref[...].T

    gw_ref[0] = mm(ht[...], g_ref[0]).astype(BF16)


def qkv_wgrad(h, g):
    rows, d = h.shape
    width = g.shape[2]
    return pl.pallas_call(
        wgrad_body,
        grid=(3,),
        in_specs=[
            pl.BlockSpec((rows, d), lambda i: (0, 0)),
            pl.BlockSpec((1, rows, width), lambda i: (i, 0, 0)),
        ],
        out_specs=pl.BlockSpec((1, d, width), lambda i: (i, 0, 0)),
        out_shape=jax.ShapeDtypeStruct((3, d, width), BF16),
        scratch_shapes=[pltpu.VMEM((d, rows), BF16)],
        compiler_params=params(),
        cost_estimate=cost(6 * rows * d * width, 8 * rows * d + 6 * d * d),
        name="qkv_wgrad",
    )(h, g)


def qkv_bwd_body(x_ref, gain_ref, w_ref, gx_ref, *refs):
    parts = refs[:-2]
    gi_ref, gn_ref = refs[-2:]

    @pl.when(pl.program_id(0) == 0)
    def _():
        gn_ref[...] = jnp.zeros_like(gn_ref)

    gh = None
    at = 0
    for part in parts:
        width = part.shape[2]
        for i in range(3):
            t = mm(part[i], w_ref[i, :, at : at + width], NT)
            gh = t if gh is None else gh + t
        at += width
    x = x_ref[...].astype(F32)
    r = rms_row(x)
    n = x * r
    gn_ref[...] += jnp.sum(gh * n, axis=0, keepdims=True)
    s = gh * gain_ref[...].astype(F32)
    gx = gx_ref[...] + r * (s - n * jnp.mean(s * n, axis=-1, keepdims=True))
    gi_ref[...] = gx.astype(BF16)


def qkv_backward(x, gain, wqkv, gx, parts):
    rows, d = x.shape
    rb = 256
    row = pl.BlockSpec((rb, d), lambda i: (i, 0))
    vec = pl.BlockSpec((1, d), lambda i: (0, 0))
    return pl.pallas_call(
        qkv_bwd_body,
        grid=(rows // rb,),
        in_specs=[row, vec, pl.BlockSpec((3, d, d), lambda i: (0, 0, 0)), row]
        + [pl.BlockSpec((3, rb, p.shape[2]), lambda i: (0, i, 0)) for p in parts],
        out_specs=[row, vec],
        out_shape=[jax.ShapeDtypeStruct((rows, d), BF16), jax.ShapeDtypeStruct((1, d), F32)],
        compiler_params=params(),
        cost_estimate=cost(6 * rows * d * d, 14 * rows * d),
        name="qkv_bwd",
    )(x, gain, wqkv, gx, *parts)


def local(
    inputs, w_query, w_key, w_value, w_out, w_gate, w_up, w_down, norm_attn, norm_ffn, lengths, cotangent,
):
    seqs, seq, d = inputs.shape
    assert seqs == 1
    x = inputs.reshape(seq, d)
    ct = cotangent.reshape(seq, d)
    cos, sin = (jnp.asarray(t) for t in rotary_lanes(seq, d // HEADS))

    def gather(w):
        return lax.all_gather(w, "fsdp", axis=0, tiled=True)

    gains = lax.all_gather(jnp.stack([norm_attn, norm_ffn]), "fsdp", axis=1, tiled=True)
    gain1 = gains[0:1]
    gain2 = gains[1:2]
    wqkv = lax.all_gather(jnp.stack([w_query, w_key, w_value]), "fsdp", axis=1, tiled=True)
    wo = gather(w_out)
    wg = gather(w_gate)
    wu = gather(w_up)
    wd = gather(w_down)

    h1, q, k, v = qkv_forward(x, gain1, wqkv, cos, sin)
    o, lse = attention_forward(lengths, q, k, v)
    x1, h2, gy = out_forward(lengths, x, o, wo, gain2, ct)
    out, gh2, gwg, gwu, gwd = ffn(h2, gy, x1, wg, wu, wd)
    gx1, go, gwo, gn2 = out_backward(gh2, x1, gy, o, wo, gain2)
    pairs = d // 128
    g = attention_backward(lengths, q, k, v, o, go, lse, cos, sin, 0, pairs)
    gwqkv = qkv_wgrad(h1, g)
    gi, gn1 = qkv_backward(x, gain1, wqkv, gx1, [g])

    def scatter(t, axis):
        return lax.psum_scatter(t, "fsdp", scatter_dimension=axis, tiled=True)

    owned = [scatter(gwqkv, 1), scatter(gwo, 0), scatter(gwg, 0), scatter(gwu, 0), scatter(gwd, 0)]
    owned = lax.psum(tuple(owned), "rep")
    norms = lax.psum(jnp.concatenate([gn1, gn2], axis=0), ("rep", "fsdp"))
    span = norm_attn.shape[0]
    mine = lax.dynamic_slice_in_dim(norms, lax.axis_index("fsdp") * span, span, axis=1)
    gqkv, gwo, gwg, gwu, gwd = (t.astype(F32) for t in owned)
    return (
        out.reshape(inputs.shape),
        gi.reshape(inputs.shape),
        gqkv[0], gqkv[1], gqkv[2],
        gwo, gwg, gwu, gwd,
        mine[0], mine[1],
    )


def solution(mesh):
    rows = P(("rep", "fsdp"), None, None)
    mat = P("fsdp", None)
    vec = P("fsdp")
    return jax.shard_map(
        local,
        mesh=mesh,
        in_specs=(rows,) + (mat,) * 7 + (vec, vec, P(("rep", "fsdp")), rows),
        out_specs=(rows, rows) + (mat,) * 7 + (vec, vec),
        check_vma=False,
    )
```
